256 devices in a mesh: near: 16 (over y, x), row: 4 (over z_hi), col: 4 (over z_lo, core).
Axes of the slice: x: 4, y: 4, z: 8 (z_hi: 4, z_lo: 2; z = z_hi * 2 + z_lo), core: 2. Of those that a mesh axis runs over, the one named last changes fastest.
Arguments:
- right_side: float32 [256, 512, 128], P(('near', 'row', 'col')), may hold values from -6 to 6
- start_guess: float32 [256, 512, 128], P(('near', 'row', 'col')), may hold values from -6 to 6
- near_tiles: bfloat16 [256, 7, 512, 512], P(('near', 'row', 'col')), may hold values from -0.09375 to 0.09375
- tile_scales: float32 [256, 7], P(('near', 'row', 'col')), may hold values from 0.3 to 3
- neighbours: int32 [256, 7], P(('near', 'row', 'col')), may hold values from 0 to 255, as said below
- source_cluster_basis: bfloat16 [256, 512, 64], P(('near', 'row', 'col')), may hold values from -0.25 to 0.25
- basis_out: bfloat16 [256, 512, 64], P(('near', 'row', 'col')), may hold values from -0.75 to 0.75
- couplings: bfloat16 [256, 256, 64, 64], P(('near', 'row'), 'col'), may hold values from -0.046875 to 0.046875
Outputs:
- solution_field: float32 [256, 512, 128], P(('near', 'row', 'col'))
- residual: float32 [256, 512, 128], P(('near', 'row', 'col'))
The draws below stay inside these ranges and needn't reach their ends.
Inputs may be any that keep to these rules, and one draw needn't show every extreme that they name: `neighbours`: row t names 7 different clusters, each within 4 of t in the wrapped cluster order.
All inputs are finite; a program needn't handle non-finite values.
Results may differ from the reference program's by a relative error of at most 0.0051.
Values may be sent and summed in bfloat16 or wider, within the bound.
No kernel may reach another device: no remote copies, remote signals or barrier semaphores. Data moves between devices by JAX's collectives and lax.ppermute only.
A program may use at most 64 MiB of HBM per device.

```python
import math
import jax
import jax.numpy as jnp
from jax import lax

LEAF = 512
RANK = 64
RHS = 128
NEIGH = 7
REACH = 4
ITERS = 2
CL_DEV = 1
CLUSTERS = 256
N_COL = 4


def draw_neighbours(key, part):
    spread = 2 * REACH + 1
    scores = jax.random.randint(key, (CLUSTERS, spread), 0, 65536)
    scores = scores * spread + jnp.arange(spread, dtype=jnp.int32)[None, :]
    ignored, picked = lax.top_k(scores, NEIGH)
    anchor_cluster = jnp.arange(CLUSTERS, dtype=jnp.int32)[:, None]
    return jnp.mod(anchor_cluster + picked.astype(jnp.int32) - REACH, CLUSTERS).astype(jnp.int32)


def block_levels(stream_key, dims, shards, least, high):
    factor_of = 1.0
    for position, shards_of in shards:
        steps = jax.random.uniform(jax.random.fold_in(jax.random.fold_in(stream_key, 6), position), (shards_of,), jnp.float32, least / len(shards), high / len(shards))
        factor_of = factor_of * jnp.repeat(jnp.exp(steps), dims[position] // shards_of).reshape((-1,) + (1,) * (len(dims) - 1 - position))
    return factor_of


def centred(key, extent, scale, most, pieces=(), kind=jnp.bfloat16):
    array = scale * jax.random.normal(key, extent, jnp.float32)
    if pieces:
        array = array * block_levels(key, extent, pieces, -0.22, 0.18)
    return jnp.clip(array, -most, most).astype(kind)


def setup_inputs(seed: int = 0) -> dict:
    splits = jax.random.split(jax.random.key(seed), 9)
    return {
        "right_side": centred(splits[0], (CLUSTERS, LEAF, RHS), 1.0, 6.0, ((0, 256),), jnp.float32),
        "start_guess": centred(splits[1], (CLUSTERS, LEAF, RHS), 1.0, 6.0, ((0, 256),), jnp.float32),
        "near_tiles": centred(splits[2], (CLUSTERS, NEIGH, LEAF, LEAF), (NEIGH * LEAF) ** -0.5, 0.09375, ((0, 256),)),
        "tile_scales": jnp.clip(jnp.exp(math.log(3.0) - 2.3025851 * jax.random.uniform(splits[3], (CLUSTERS, NEIGH), jnp.float32) ** block_levels(splits[3], (CLUSTERS, NEIGH), ((0, 256),), -0.2, 0.2)), 0.3, 3.0),
        "neighbours": draw_neighbours(jax.random.fold_in(splits[8], 71), 0),
        "source_cluster_basis": centred(splits[5], (CLUSTERS, LEAF, RANK), LEAF ** -0.5, 0.25, ((0, 256),)),
        "basis_out": centred(splits[6], (CLUSTERS, LEAF, RANK), RANK ** -0.5, 0.75, ((0, 256),)),
        "couplings": centred(splits[7], (CLUSTERS, CLUSTERS, RANK, RANK), (CLUSTERS * RANK) ** -0.5, 0.046875, ((0, 64), (1, 4))),
    }


damping = 0.5


def slot_owner(slot_ids):
    per_col = CLUSTERS // N_COL
    within = slot_ids % per_col
    column = slot_ids // per_col
    return (within // CL_DEV * N_COL + column) * CL_DEV + within % CL_DEV


def far_pairs(targets, sources):
    distance = jnp.mod(targets[:, None] - sources[None, :], CLUSTERS)
    return jnp.minimum(distance, CLUSTERS - distance) > REACH


def operate(vector, near_tiles, tile_scales, neighbours, source_cluster_basis, basis_out, couplings):
    coarse_level = vector.astype(jnp.bfloat16)
    expansion_coefficients = jnp.einsum("iao,iau->iou", source_cluster_basis.astype(jnp.float32), coarse_level.astype(jnp.float32),
                       precision=lax.Precision.HIGHEST).astype(jnp.bfloat16)

    def near_one(item):
        tile_set, scale_set, index_set = item
        nearby = jnp.take(coarse_level, index_set, axis=0).astype(jnp.float32)
        basis_products = jnp.einsum("jkl,jlc->jkc", tile_set.astype(jnp.float32), nearby,
                              precision=lax.Precision.HIGHEST)
        return jnp.sum(basis_products * scale_set[:, None, None], axis=0)

    near_term = lax.map(near_one, (near_tiles, tile_scales, neighbours))
    slot_ids = jnp.arange(CLUSTERS, dtype=jnp.int32)
    owners = slot_owner(slot_ids)
    slot_coefs = jnp.take(expansion_coefficients, owners, axis=0).astype(jnp.float32)

    def far_one(item):
        coupling_row, target = item
        admitted = far_pairs(target[None], owners)[0].astype(jnp.float32)
        masked_values = coupling_row.astype(jnp.float32) * admitted[:, None, None]
        return jnp.einsum("mab,mbc->ac", masked_values, slot_coefs, precision=lax.Precision.HIGHEST)

    farfield_coefficients = lax.map(far_one, (couplings, slot_ids))
    far_term = jnp.einsum("cla,cad->cld", basis_out.astype(jnp.float32),
                          farfield_coefficients.astype(jnp.bfloat16).astype(jnp.float32),
                          precision=lax.Precision.HIGHEST)
    return vector + near_term + far_term


def reference(right_side, start_guess, near_tiles, tile_scales, neighbours, source_cluster_basis, basis_out, couplings):
    iterate = start_guess
    residual = right_side
    for sweep in range(ITERS):
        residual = right_side - operate(iterate, near_tiles, tile_scales, neighbours, source_cluster_basis, basis_out, couplings)
        iterate = iterate + damping * residual
    return iterate, residual
```

```python
import jax
import jax.numpy as jnp
from jax import lax
from jax.experimental import pallas as pl
from jax.experimental.pallas import tpu as pltpu
from jax.sharding import PartitionSpec as P

REACH = 4
ITERS = 2
ALL = ("near", "row", "col")

damping = 0.5

SLOTS = (8, 6, 7, 1, 0, 3, 2, 5, 4)


def moved(value, target):
    count = lax.axis_size(ALL)
    return lax.ppermute(value, ALL, [(source, target(source) % count) for source in range(count)])


def outward(steps):
    return lambda source: source + steps if source % 2 == 0 else source - steps


def partner(source):
    return source ^ 1


def sent_to_all(array, axis):
    copies = jnp.broadcast_to(array, (lax.axis_size(axis), *array.shape))
    return lax.all_to_all(copies, axis, split_axis=0, concat_axis=0, tiled=True)


def near_body(slots, scales, tiles, own, other, first, second, back, out, window):
    step = pl.program_id(0)

    @pl.when(step == 0)
    def _():
        window[0] = own[...]
        window[1] = other[...]
        window[2:4] = first[...]
        window[4:6] = second[...]
        window[6:9] = back[...]

    product = scales[step] * jnp.dot(
        tiles[0], window[slots[step]], preferred_element_type=jnp.float32
    )

    @pl.when(step == 0)
    def _():
        out[...] = product

    @pl.when(step > 0)
    def _():
        out[...] += product


def near_product(slots, scales, tiles, own, other, first, second, back):
    count, rows, inner = tiles.shape
    cols = own.shape[-1]

    def whole(array):
        return pl.BlockSpec(array.shape, lambda k, *_: (0,) * array.ndim)

    return pl.pallas_call(
        near_body,
        out_shape=jax.ShapeDtypeStruct((rows, cols), jnp.float32),
        grid_spec=pltpu.PrefetchScalarGridSpec(
            num_scalar_prefetch=2,
            grid=(count,),
            in_specs=[
                pl.BlockSpec((1, rows, inner), lambda k, *_: (k, 0, 0)),
                whole(own),
                whole(other),
                whole(first),
                whole(second),
                whole(back),
            ],
            out_specs=pl.BlockSpec((rows, cols), lambda k, *_: (0, 0)),
            scratch_shapes=[pltpu.VMEM((2 * REACH + 1, rows, cols), own.dtype)],
        ),
        cost_estimate=pl.CostEstimate(
            flops=2 * count * rows * inner * cols,
            bytes_accessed=2 * count * rows * inner,
            transcendentals=0,
        ),
        name="near",
    )(slots, scales, tiles, own, other, first, second, back)


def halo(own):
    other = moved(own, partner)
    pair = jnp.stack([own, other])
    first = moved(pair, outward(2))
    second = moved(pair, outward(4))
    back = moved(jnp.concatenate([first, second[1:]]), partner)
    return own, other, first, second, back


def shards(
    right_side,
    start_guess,
    near_tiles,
    tile_scales,
    neighbours,
    source_cluster_basis,
    basis_out,
    couplings,
):
    right_side, iterate = right_side[0], start_guess[0]
    near_tiles, scales = near_tiles[0], tile_scales[0]
    basis_in, basis_out = source_cluster_basis[0], basis_out[0]
    clusters = lax.axis_size(ALL)
    col_count = lax.axis_size("col")
    col_index = lax.axis_index("col")
    group_index = lax.axis_index(("near", "row"))
    device = lax.axis_index(ALL)
    side = 2 * (device % 2) - 1
    offsets = jnp.mod(neighbours[0] - device + REACH, clusters) - REACH
    places = jnp.arange(2 * REACH + 1, dtype=jnp.int32)
    chosen = (side * offsets + REACH)[:, None] == places[None, :]
    slots = jnp.sum(jnp.where(chosen, jnp.array(SLOTS, jnp.int32)[None, :], 0), axis=1)

    targets, sources, rank, _ = couplings.shape
    block_targets = group_index * targets + jnp.arange(targets, dtype=jnp.int32)
    block_sources = jnp.arange(sources, dtype=jnp.int32) * col_count + col_index
    distance = jnp.mod(block_targets[:, None] - block_sources[None, :], clusters)
    admitted = (jnp.minimum(distance, clusters - distance) > REACH).astype(couplings.dtype)
    masked = couplings * admitted[:, :, None, None]
    far_rows = jnp.transpose(masked, (0, 2, 1, 3)).reshape(targets * rank, sources * rank)
    far_rows = lax.optimization_barrier(far_rows)

    residual = right_side
    for sweep in range(ITERS):
        coarse = iterate.astype(jnp.bfloat16)
        coefs = jnp.einsum(
            "lr,lc->rc", basis_in, coarse, preferred_element_type=jnp.float32
        ).astype(jnp.bfloat16)
        gathered = sent_to_all(sent_to_all(coefs, "row"), "near")
        near_term = near_product(slots, scales, near_tiles, *halo(coarse))
        partial_coefs = jnp.dot(
            far_rows, gathered.reshape(sources * rank, -1), preferred_element_type=jnp.float32
        ).astype(jnp.bfloat16)
        pieces = lax.all_to_all(
            partial_coefs.reshape(targets, rank, -1), "col", 0, 0, tiled=True
        )
        far_coefs = jnp.sum(pieces.astype(jnp.float32), axis=0).astype(jnp.bfloat16)
        far_term = jnp.dot(basis_out, far_coefs, preferred_element_type=jnp.float32)
        residual = right_side - (iterate + near_term + far_term)
        iterate = iterate + damping * residual
    return (iterate[None], residual[None])


def solution(mesh):
    in_specs = (
        P(ALL, None, None),
        P(ALL, None, None),
        P(ALL, None, None, None),
        P(ALL, None),
        P(ALL, None),
        P(ALL, None, None),
        P(ALL, None, None),
        P(("near", "row"), "col", None, None),
    )
    out_specs = (P(ALL, None, None), P(ALL, None, None))
    return jax.shard_map(shards, mesh=mesh, in_specs=in_specs, out_specs=out_specs, check_vma=False)
```

```python
import jax
import jax.numpy as jnp
from jax import lax
from jax.experimental import pallas as pl
from jax.experimental.pallas import tpu as pltpu
from jax.sharding import PartitionSpec as P

REACH = 4
ITERS = 2
ALL = ("near", "row", "col")

damping = 0.5

SLOTS = (8, 6, 7, 1, 0, 3, 2, 5, 4)
ROW_STEPS = (0, -1, 1, 2)


def moved(value, target):
    count = lax.axis_size(ALL)
    return lax.ppermute(value, ALL, [(source, target(source) % count) for source in range(count)])


def outward(steps):
    return lambda source: source + steps if source % 2 == 0 else source - steps


def crossed(mask):
    return lambda source: source ^ mask


def along_row(value, steps):
    count = lax.axis_size("row")
    return lax.ppermute(value, "row", [(source, (source + steps) % count) for source in range(count)])


def sent_to_all(array, axis):
    copies = jnp.broadcast_to(array, (lax.axis_size(axis), *array.shape))
    return lax.all_to_all(copies, axis, split_axis=0, concat_axis=0, tiled=True)


SMEM = pltpu.MemorySpace.SMEM
HBM = pltpu.MemorySpace.HBM


def base_body(
    slots, scales, tiles, own, other, first, second, back, right, iterate, out,
    tile_buf, window, right_buf, iterate_buf, tile_sems, sems,
):
    count = tiles.shape[0]
    copies = [
        pltpu.make_async_copy(own, window.at[0], sems.at[0]),
        pltpu.make_async_copy(other, window.at[1], sems.at[1]),
        pltpu.make_async_copy(first, window.at[pl.ds(2, 2)], sems.at[2]),
        pltpu.make_async_copy(second, window.at[pl.ds(4, 2)], sems.at[3]),
        pltpu.make_async_copy(back, window.at[pl.ds(6, 3)], sems.at[4]),
    ]
    tile_copies = [
        pltpu.make_async_copy(tiles.at[k], tile_buf.at[k], tile_sems.at[k]) for k in range(count)
    ]
    vector_copies = [
        pltpu.make_async_copy(right, right_buf, sems.at[5]),
        pltpu.make_async_copy(iterate, iterate_buf, sems.at[6]),
    ]
    for copy in copies + tile_copies + vector_copies:
        copy.start()
    for copy in copies:
        copy.wait()
    for k in range(count):
        tile_copies[k].wait()
        product = scales[k] * jnp.dot(
            tile_buf[k], window[slots[k]], preferred_element_type=jnp.float32
        )
        out[...] = product if k == 0 else out[...] + product
    for copy in vector_copies:
        copy.wait()
    out[...] = right_buf[...] - (iterate_buf[...] + out[...])


def base_residual(slots, scales, tiles, own, other, first, second, back, right, iterate):
    count, rows, inner = tiles.shape
    cols = own.shape[-1]
    hbm = pl.BlockSpec(memory_space=HBM)
    smem = pl.BlockSpec(memory_space=SMEM)
    return pl.pallas_call(
        base_body,
        out_shape=jax.ShapeDtypeStruct((rows, cols), jnp.float32),
        in_specs=[smem, smem] + [hbm] * 8,
        out_specs=pl.BlockSpec(memory_space=pltpu.MemorySpace.VMEM),
        scratch_shapes=[
            pltpu.VMEM((count, rows, inner), tiles.dtype),
            pltpu.VMEM((2 * REACH + 1, rows, cols), own.dtype),
            pltpu.VMEM((rows, cols), jnp.float32),
            pltpu.VMEM((rows, cols), jnp.float32),
            pltpu.SemaphoreType.DMA((count,)),
            pltpu.SemaphoreType.DMA((7,)),
        ],
        cost_estimate=pl.CostEstimate(
            flops=2 * count * rows * inner * cols,
            bytes_accessed=2 * count * rows * inner,
            transcendentals=0,
        ),
        name="near",
    )(slots, scales, tiles, own, other, first, second, back, right, iterate)


def layout_body(place, couplings, out, *, clusters, rows):
    group, row, col = place[0], place[1], place[2]
    targets, block, rank, _ = couplings.shape
    step = pl.program_id(0)
    for part in range(block // rows):
        for m in range(targets):
            local = col ^ m
            target = group * targets + local
            pieces = []
            for distance in ROW_STEPS:
                within = part * rows + (row + distance + rows) % rows
                source = (step * block + within) * targets + col
                gap = (target - source + clusters) % clusters
                far = jnp.minimum(gap, clusters - gap) > REACH
                piece = couplings[local, within]
                pieces.append(jnp.where(far, piece, jnp.zeros_like(piece)))
            out[m * rank : (m + 1) * rank, part * rows * rank : (part + 1) * rows * rank] = (
                jnp.concatenate(pieces, axis=1)
            )


def laid_out_couplings(place, couplings, clusters, rows):
    targets, sources, rank, _ = couplings.shape
    block = 4 * rows
    return pl.pallas_call(
        lambda *refs: layout_body(*refs, clusters=clusters, rows=rows),
        out_shape=jax.ShapeDtypeStruct((targets * rank, sources * rank), couplings.dtype),
        grid=(sources // block,),
        in_specs=[
            pl.BlockSpec(memory_space=SMEM),
            pl.BlockSpec((targets, block, rank, rank), lambda k: (0, k, 0, 0)),
        ],
        out_specs=pl.BlockSpec((targets * rank, block * rank), lambda k: (0, k)),
        cost_estimate=pl.CostEstimate(
            flops=0, bytes_accessed=6 * targets * sources * rank * rank, transcendentals=0
        ),
        name="layout",
    )(place, couplings)


def halo(own):
    other = moved(own, crossed(1))
    pair = jnp.stack([own, other])
    first = moved(pair, outward(2))
    second = moved(pair, outward(4))
    back = moved(jnp.concatenate([first, second[1:]]), crossed(1))
    return own, other, first, second, back


def shards(
    right_side,
    start_guess,
    near_tiles,
    tile_scales,
    neighbours,
    source_cluster_basis,
    basis_out,
    couplings,
):
    right_side, iterate = right_side[0], start_guess[0]
    near_tiles, scales = near_tiles[0], tile_scales[0]
    basis_in, basis_out = source_cluster_basis[0], basis_out[0]
    clusters = lax.axis_size(ALL)
    row_count = lax.axis_size("row")
    device = lax.axis_index(ALL)
    side = 2 * (device % 2) - 1
    offsets = jnp.mod(neighbours[0] - device + REACH, clusters) - REACH
    places = jnp.arange(2 * REACH + 1, dtype=jnp.int32)
    chosen = (side * offsets + REACH)[:, None] == places[None, :]
    slots = jnp.sum(jnp.where(chosen, jnp.array(SLOTS, jnp.int32)[None, :], 0), axis=1)

    targets, sources, rank, _ = couplings.shape
    place = jnp.stack([lax.axis_index(("near", "row")), lax.axis_index("row"), lax.axis_index("col")])
    far_rows = laid_out_couplings(place.astype(jnp.int32), couplings, clusters, row_count)

    residual = right_side
    for sweep in range(ITERS):
        coarse = iterate.astype(jnp.bfloat16)
        coefs = jnp.einsum(
            "lr,lc->rc", basis_in, coarse, preferred_element_type=jnp.float32
        ).astype(jnp.bfloat16)
        in_row = jnp.stack(
            [along_row(coefs, -steps) if steps else coefs for steps in ROW_STEPS]
        )
        gathered = sent_to_all(in_row, "near")
        base = base_residual(slots, scales, near_tiles, *halo(coarse), right_side, iterate)
        partial_coefs = (
            jnp.dot(
                far_rows, gathered.reshape(sources * rank, -1), preferred_element_type=jnp.float32
            )
            .astype(jnp.bfloat16)
            .reshape(targets, rank, -1)
        )
        far_coefs = partial_coefs[0].astype(jnp.float32)
        for m in range(1, targets):
            far_coefs += moved(partial_coefs[m], crossed(m)).astype(jnp.float32)
        far_term = jnp.dot(
            basis_out, far_coefs.astype(jnp.bfloat16), preferred_element_type=jnp.float32
        )
        residual = base - far_term
        iterate = iterate + damping * residual
    return (iterate[None], residual[None])


def solution(mesh):
    in_specs = (
        P(ALL, None, None),
        P(ALL, None, None),
        P(ALL, None, None, None),
        P(ALL, None),
        P(ALL, None),
        P(ALL, None, None),
        P(ALL, None, None),
        P(("near", "row"), "col", None, None),
    )
    out_specs = (P(ALL, None, None), P(ALL, None, None))
    return jax.shard_map(shards, mesh=mesh, in_specs=in_specs, out_specs=out_specs, check_vma=False)
```

```python
import jax
import jax.numpy as jnp
from jax import lax
from jax.experimental import pallas as pl
from jax.experimental.pallas import tpu as pltpu
from jax.sharding import PartitionSpec as P

REACH = 4
ITERS = 2
ALL = ("near", "row", "col")

damping = 0.5

SLOTS = (8, 6, 7, 1, 0, 3, 2, 5, 4)
ROW_STEPS = (0, -1, 1, 2)
BLOCK = 128


def moved(value, target):
    count = lax.axis_size(ALL)
    return lax.ppermute(value, ALL, [(source, target(source) % count) for source in range(count)])


def outward(steps):
    return lambda source: source + steps if source % 2 == 0 else source - steps


def crossed(mask):
    return lambda source: source ^ mask


def along_row(value, steps):
    count = lax.axis_size("row")
    return lax.ppermute(value, "row", [(source, (source + steps) % count) for source in range(count)])


def sent_to_all(array, axis):
    copies = jnp.broadcast_to(array, (lax.axis_size(axis), *array.shape))
    return lax.all_to_all(copies, axis, split_axis=0, concat_axis=0, tiled=True)


SMEM = pltpu.MemorySpace.SMEM
HBM = pltpu.MemorySpace.HBM


def base_body(
    slots, scales, tiles, own, other, first, second, back, right, iterate, out,
    tile_buf, window, right_buf, iterate_buf, tile_sems, sems,
):
    count = tiles.shape[0]
    copies = [
        pltpu.make_async_copy(own, window.at[0], sems.at[0]),
        pltpu.make_async_copy(other, window.at[1], sems.at[1]),
        pltpu.make_async_copy(first, window.at[pl.ds(2, 2)], sems.at[2]),
        pltpu.make_async_copy(second, window.at[pl.ds(4, 2)], sems.at[3]),
        pltpu.make_async_copy(back, window.at[pl.ds(6, 3)], sems.at[4]),
    ]
    tile_copies = [
        pltpu.make_async_copy(tiles.at[k], tile_buf.at[k], tile_sems.at[k]) for k in range(count)
    ]
    vector_copies = [
        pltpu.make_async_copy(right, right_buf, sems.at[5]),
        pltpu.make_async_copy(iterate, iterate_buf, sems.at[6]),
    ]
    for copy in copies + tile_copies + vector_copies:
        copy.start()
    for copy in copies:
        copy.wait()
    for copy in vector_copies:
        copy.wait()
    for copy in tile_copies:
        copy.wait()
    for start in range(0, out.shape[0], BLOCK):
        block = pl.ds(start, BLOCK)
        total = None
        for k in range(count):
            product = scales[k] * jnp.dot(
                tile_buf[k, block], window[slots[k]], preferred_element_type=jnp.float32
            )
            total = product if total is None else total + product
        out[block] = right_buf[block] - (iterate_buf[block] + total)


def base_residual(slots, scales, tiles, own, other, first, second, back, right, iterate):
    count, rows, inner = tiles.shape
    cols = own.shape[-1]
    hbm = pl.BlockSpec(memory_space=HBM)
    smem = pl.BlockSpec(memory_space=SMEM)
    return pl.pallas_call(
        base_body,
        out_shape=jax.ShapeDtypeStruct((rows, cols), jnp.float32),
        in_specs=[smem, smem] + [hbm] * 8,
        out_specs=pl.BlockSpec(memory_space=pltpu.MemorySpace.VMEM),
        scratch_shapes=[
            pltpu.VMEM((count, rows, inner), tiles.dtype),
            pltpu.VMEM((2 * REACH + 1, rows, cols), own.dtype),
            pltpu.VMEM((rows, cols), jnp.float32),
            pltpu.VMEM((rows, cols), jnp.float32),
            pltpu.SemaphoreType.DMA((count,)),
            pltpu.SemaphoreType.DMA((7,)),
        ],
        cost_estimate=pl.CostEstimate(
            flops=2 * count * rows * inner * cols,
            bytes_accessed=2 * count * rows * inner,
            transcendentals=0,
        ),
        name="near",
    )(slots, scales, tiles, own, other, first, second, back, right, iterate)


def layout_body(place, couplings, out, *, clusters, rows):
    group, row, col = place[0], place[1], place[2]
    targets, block, rank, _ = couplings.shape
    step = pl.program_id(0)
    for part in range(block // rows):
        for m in range(targets):
            local = col ^ m
            target = group * targets + local
            pieces = []
            for distance in ROW_STEPS:
                within = part * rows + (row + distance + rows) % rows
                source = (step * block + within) * targets + col
                gap = (target - source + clusters) % clusters
                far = jnp.minimum(gap, clusters - gap) > REACH
                piece = couplings[local, within]
                pieces.append(jnp.where(far, piece, jnp.zeros_like(piece)))
            out[m * rank : (m + 1) * rank, part * rows * rank : (part + 1) * rows * rank] = (
                jnp.concatenate(pieces, axis=1)
            )


def laid_out_couplings(place, couplings, clusters, rows):
    targets, sources, rank, _ = couplings.shape
    block = 4 * rows
    return pl.pallas_call(
        lambda *refs: layout_body(*refs, clusters=clusters, rows=rows),
        out_shape=jax.ShapeDtypeStruct((targets * rank, sources * rank), couplings.dtype),
        grid=(sources // block,),
        in_specs=[
            pl.BlockSpec(memory_space=SMEM),
            pl.BlockSpec((targets, block, rank, rank), lambda k: (0, k, 0, 0)),
        ],
        out_specs=pl.BlockSpec((targets * rank, block * rank), lambda k: (0, k)),
        cost_estimate=pl.CostEstimate(
            flops=0, bytes_accessed=6 * targets * sources * rank * rank, transcendentals=0
        ),
        name="layout",
    )(place, couplings)


def halo(own):
    other = moved(own, crossed(1))
    pair = jnp.stack([own, other])
    first = moved(pair, outward(2))
    second = moved(pair, outward(4))
    back = moved(jnp.concatenate([first, second[1:]]), crossed(1))
    return own, other, first, second, back


def in_row(coefs):
    held = []
    for steps in ROW_STEPS:
        held.append(along_row(coefs, -steps) if steps else coefs)
    return jnp.stack(held)


def one_sweep(iterate, right_side, slots, scales, near_tiles, basis_in, basis_out, far_rows, targets):
    coarse = iterate.astype(jnp.bfloat16)
    coefs = jnp.einsum(
        "lr,lc->rc", basis_in, coarse, preferred_element_type=jnp.float32
    ).astype(jnp.bfloat16)
    rank, cols = coefs.shape
    held = in_row(coefs)
    gathered = sent_to_all(held, "near")
    base = base_residual(slots, scales, near_tiles, *halo(coarse), right_side, iterate)
    partial_coefs = jnp.dot(
        far_rows, gathered.reshape(-1, cols), preferred_element_type=jnp.float32
    )
    partial_coefs = partial_coefs.astype(jnp.bfloat16).reshape(targets, rank, cols)
    far_coefs = partial_coefs[0].astype(jnp.float32)
    for m in range(1, targets):
        arrived = moved(partial_coefs[m], crossed(m))
        far_coefs += arrived.astype(jnp.float32)
    far_term = jnp.dot(
        basis_out, far_coefs.astype(jnp.bfloat16), preferred_element_type=jnp.float32
    )
    residual = base - far_term
    return iterate + damping * residual, residual


def shards(
    right_side,
    start_guess,
    near_tiles,
    tile_scales,
    neighbours,
    source_cluster_basis,
    basis_out,
    couplings,
):
    right_side, iterate = right_side[0], start_guess[0]
    near_tiles, scales = near_tiles[0], tile_scales[0]
    basis_in, basis_out = source_cluster_basis[0], basis_out[0]
    clusters = lax.axis_size(ALL)
    row_count = lax.axis_size("row")
    device = lax.axis_index(ALL)
    side = 2 * (device % 2) - 1
    offsets = jnp.mod(neighbours[0] - device + REACH, clusters) - REACH
    places = jnp.arange(2 * REACH + 1, dtype=jnp.int32)
    chosen = (side * offsets + REACH)[:, None] == places[None, :]
    slots = jnp.sum(jnp.where(chosen, jnp.array(SLOTS, jnp.int32)[None, :], 0), axis=1)

    targets, _, _, _ = couplings.shape
    place = jnp.stack([lax.axis_index(("near", "row")), lax.axis_index("row"), lax.axis_index("col")])
    far_rows = laid_out_couplings(place.astype(jnp.int32), couplings, clusters, row_count)

    residual = right_side
    for _ in range(ITERS):
        iterate, residual = one_sweep(
            iterate, right_side, slots, scales, near_tiles, basis_in, basis_out, far_rows, targets
        )
    return (iterate[None], residual[None])


def solution(mesh):
    in_specs = (
        P(ALL, None, None),
        P(ALL, None, None),
        P(ALL, None, None, None),
        P(ALL, None),
        P(ALL, None),
        P(ALL, None, None),
        P(ALL, None, None),
        P(("near", "row"), "col", None, None),
    )
    out_specs = (P(ALL, None, None), P(ALL, None, None))
    return jax.shard_map(shards, mesh=mesh, in_specs=in_specs, out_specs=out_specs, check_vma=False)
```
